32 devices in a mesh: cell: 8 (over z, x), gene: 4 (over y, core).
Axes of the slice: x: 2, y: 2, z: 4, core: 2. Of those that a mesh axis runs over, the one named last changes fastest.
Arguments:
- counts: int32 [2048, 4096], P('cell', 'gene'), may hold values from 0 to 7
- totals: int32 [2048], P('cell'), may hold values from 1000 to 19999
- cell_factors: float32 [2048, 32], P('cell'), may hold values from -0.9 to 0.9
- gene_loadings: float32 [4096, 32], P('gene'), may hold values from -0.9 to 0.9
Outputs:
- new_factors: float32 [2048, 32], P('cell')
- new_loadings: float32 [4096, 32], P('gene')
- deviance: float32 [4096], P('gene')
The draws below stay inside these ranges and needn't reach their ends.
All inputs are finite; a program needn't handle non-finite values.
Results may differ from the reference program's by a relative error of at most 0.0044.
Values sent between devices are 32-bit elements; how exact they have to be, the bound alone decides.
A program may use at most 128 MiB of HBM per device.

```python
import math
import jax
import jax.numpy as jnp
from jax import lax

L = 32
GENES = 4096
CD = 256
CELLS = 2048
N_CELL = 8


def set_ends(result, rng, smallest, largest):
    shape = result.shape
    place = [jax.random.randint(jax.random.fold_in(rng, axis), (), 0, shape[axis]) for axis in range(len(shape))]
    result = result.at[tuple(place)].set(smallest)
    longest = shape.index(max(shape))
    place[longest] = (place[longest] + 1) % shape[longest]
    return result.at[tuple(place)].set(largest)


def block_levels(stream_key, shape, shards, smallest, top_value):
    gain = 1.0
    for dim, parts in shards:
        draws = jax.random.uniform(jax.random.fold_in(jax.random.fold_in(stream_key, 6), dim), (parts,), jnp.float32, smallest / len(shards), top_value / len(shards))
        gain = gain * jnp.repeat(jnp.exp(draws), shape[dim] // parts).reshape((-1,) + (1,) * (len(shape) - 1 - dim))
    return gain


def gaussian(rng, extent, deviation, bound, shards=(), dtype=jnp.bfloat16):
    result = deviation * jax.random.normal(rng, extent, jnp.float32)
    if shards:
        result = result * block_levels(rng, extent, shards, -0.22, 0.18)
    return jnp.clip(result, -bound, bound).astype(dtype)


def setup_inputs(seed: int = 0) -> dict:
    keys = jax.random.split(jax.random.key(seed), 5)
    counts = set_ends(jax.random.randint(keys[0], (CELLS, GENES), 0, 8), jax.random.fold_in(keys[0], 1), 0, 7).astype(jnp.int32)
    totals = set_ends(jax.random.randint(keys[1], (CELLS,), 1000, 20000), jax.random.fold_in(keys[1], 1), 1000, 19999).astype(jnp.int32)
    cell_factors = gaussian(keys[2], (CELLS, L), 0.15, 0.9, ((0, 8),), jnp.float32)
    gene_loadings = gaussian(keys[3], (GENES, L), 0.15, 0.9, ((0, 4),), jnp.float32)
    return {"counts": counts, "totals": totals, "cell_factors": cell_factors, "gene_loadings": gene_loadings}


RIDGE = 1.0
DAMPING = 0.1
SCALE_TOTAL = 5000.0

def outer_table(factors):
    width = factors.shape[1]
    product = factors[:, :, None] * factors[:, None, :]
    return product.reshape(factors.shape[0], width * width).astype(jnp.bfloat16)

def newton_solve(curvature, gradient):
    width = gradient.shape[1]
    matrix = jnp.transpose(curvature.reshape(gradient.shape[0], width, width), (1, 2, 0))
    diagonal_mean = sum((matrix[index, index] for index in range(width))) / width
    shift = RIDGE + DAMPING * diagonal_mean
    right = jnp.transpose(gradient)
    columns = []
    for column in range(width):
        current = matrix[:, column]
        if column > 0:
            stacked = jnp.stack(columns)
            current = current - lax.optimization_barrier(jnp.sum(stacked * stacked[:, column][:, None, :], axis=0))
        current = current + jnp.where(jnp.arange(width) == column, 1.0, 0.0).astype(jnp.float32)[:, None] * shift[None, :]
        pivot = jnp.sqrt(current[column])
        mask = (jnp.arange(width) >= column).astype(jnp.float32)[:, None]
        columns.append(mask * current / pivot[None, :])
    lower = jnp.stack(columns, axis=1)
    forward = []
    for row in range(width):
        value = right[row]
        for inner in range(row):
            value = value - lower[row, inner] * forward[inner]
        forward.append(value / lower[row, row])
    backward = [None] * width
    for row in range(width - 1, -1, -1):
        value = forward[row]
        for inner in range(row + 1, width):
            value = value - lower[inner, row] * backward[inner]
        backward[row] = value / lower[row, row]
    return jnp.transpose(jnp.stack(backward))

def predict(offset, factors, loadings):
    linear = offset[:, None] + jnp.dot(factors, loadings.T, precision=lax.Precision.HIGHEST)
    return (linear, jnp.exp(linear))

def gene_contract(counts, expected, loadings):
    weights = expected.astype(jnp.bfloat16)
    residual = (counts.astype(jnp.float32) - expected).astype(jnp.bfloat16)
    gradient = jnp.dot(residual, loadings.astype(jnp.bfloat16), preferred_element_type=jnp.float32)
    curvature = jnp.dot(weights, outer_table(loadings), preferred_element_type=jnp.float32)
    return (gradient, curvature)

def cell_contract(counts, linear, expected, factors):
    counts_real = counts.astype(jnp.float32)
    weights = expected.astype(jnp.bfloat16)
    residual = (counts_real - expected).astype(jnp.bfloat16)
    dims = (((0,), (0,)), ((), ()))
    gradient = lax.dot_general(residual, factors.astype(jnp.bfloat16), dims, preferred_element_type=jnp.float32)
    curvature = lax.dot_general(weights, outer_table(factors), dims, preferred_element_type=jnp.float32)
    terms = 2.0 * (counts_real * (jnp.log(jnp.maximum(counts_real, 1.0)) - linear) - counts_real + expected)
    return (gradient, curvature, lax.optimization_barrier(jnp.sum(terms, axis=0)))

def reference(counts, totals, cell_factors, gene_loadings):
    offset = jnp.log(totals.astype(jnp.float32)) - math.log(SCALE_TOTAL)
    count_blocks = counts.reshape(N_CELL, CD, GENES)
    offset_blocks = offset.reshape(N_CELL, CD)
    factor_blocks = cell_factors.reshape(N_CELL, CD, L)

    def factor_update(block):
        count_block, offset_block, factor_block = block
        linear, expected = predict(offset_block, factor_block, gene_loadings)
        gradient, curvature = gene_contract(count_block, expected, gene_loadings)
        return factor_block + newton_solve(curvature, gradient - RIDGE * factor_block)
    new_blocks = lax.map(factor_update, (count_blocks, offset_blocks, factor_blocks))
    new_factors = new_blocks.reshape(CELLS, L)

    def loading_update(running, block):
        count_block, offset_block, factor_block = block
        linear, expected = predict(offset_block, factor_block, gene_loadings)
        gradient, curvature, deviance_part = cell_contract(count_block, linear, expected, factor_block)
        return ((running[0] + gradient, running[1] + curvature, running[2] + deviance_part), None)
    initial = (jnp.zeros((GENES, L), jnp.float32), jnp.zeros((GENES, L * L), jnp.float32), jnp.zeros((GENES,), jnp.float32))
    totals_sum, unused = lax.scan(loading_update, initial, (count_blocks, offset_blocks, new_blocks))
    gradient_sum, curvature_sum, deviance_sum = totals_sum
    new_loadings = gene_loadings + newton_solve(curvature_sum, gradient_sum - RIDGE * gene_loadings)
    deviance = deviance_sum / CELLS
    return (new_factors, new_loadings, deviance)
```

```python
import functools
import math

import jax
import jax.numpy as jnp
from jax import lax
from jax.experimental import pallas as pl
from jax.experimental.pallas import tpu as pltpu
from jax.sharding import PartitionSpec as P

RIDGE = 1.0
DAMPING = 0.1
SCALE_TOTAL = 5000.0
LANES = 128
SUB = 8
BLOCK = 256
HIGH = lax.Precision.HIGHEST
NT = (((1,), (1,)), ((), ()))
LOG2E = 1.0 / math.log(2.0)
F32 = jnp.float32
BF16 = jnp.bfloat16


def packed_rows(width):
    return sum(width - SUB * (a // SUB) for a in range(width))


def lower_table(factors):
    width = factors.shape[0]
    pieces = [factors[a : a + 1] * factors[SUB * (a // SUB) :] for a in range(width)]
    return jnp.concatenate(pieces, axis=0).astype(BF16)


def split3(x):
    first = x.astype(BF16)
    rest = x - first.astype(F32)
    second = rest.astype(BF16)
    third = (rest - second.astype(F32)).astype(BF16)
    return first, second, third


def rows_of(value, count):
    index = lax.broadcasted_iota(jnp.int32, (2 * SUB, count), 0)
    parts = [x.astype(F32) for x in value] if isinstance(value, tuple) else [value] * 3
    result = jnp.zeros((2 * SUB, count), F32)
    for place, part in enumerate(parts):
        result = jnp.where(index == place, part, result)
    return result.astype(BF16)


def fixed_side(rows, tail):
    first, second, third = (x.astype(F32) for x in split3(rows))
    stack = jnp.concatenate([first, first, second, first, third, second, tail.astype(F32)], axis=0)
    return jnp.transpose(stack).astype(BF16)


def stream_side(rows, tail):
    first, second, third = split3(rows)
    return jnp.concatenate([first, second, first, third, first, second, tail], axis=0), first


def table_of(rows, first):
    width, count = rows.shape
    ones = jnp.where(lax.broadcasted_iota(jnp.int32, (2 * SUB, count), 0) == 0, 1.0, 0.0).astype(BF16)
    return jnp.concatenate([lower_table(rows), first, ones], axis=0)


def accumulate(left, rows, tail):
    width = rows.shape[0]
    right, first = stream_side(rows, tail)
    expected = jnp.exp2(jnp.dot(left, right, preferred_element_type=F32))
    high = expected.astype(BF16)
    low = (expected - high.astype(F32)).astype(BF16)
    table = table_of(rows, first)
    sums = lax.dot_general(table, high, NT, preferred_element_type=F32)
    extra = lax.dot_general(table[packed_rows(width) :], low, NT, preferred_element_type=F32)
    return sums, extra


def solve_packed(get, right, width):
    columns, start = [], 0
    for a in range(width):
        rows = width - SUB * (a // SUB)
        columns.append(get(start, rows))
        start += rows
    diagonal = sum(columns[a][a % SUB : a % SUB + 1] for a in range(width)) / width
    shift = RIDGE + DAMPING * diagonal
    count = width // SUB
    index = lax.broadcasted_iota(jnp.int32, (width, right.shape[1]), 0)
    lower, scaled = [], []
    value = right
    for a in range(width):
        own, place = a // SUB, a % SUB
        column = columns[a]
        rows = index[: width - SUB * own]
        inverse = 1.0 / (column[place : place + 1] + shift)
        factor = jnp.where(rows > place, column * inverse, 0.0)
        for b in range(a + 1, width):
            offset = SUB * (b // SUB - own)
            coefficient = column[b - SUB * own : b - SUB * own + 1]
            columns[b] = columns[b] - factor[offset:] * coefficient
        lower.append(factor)
        head = value[SUB * own :]
        pivot = head[place : place + 1]
        scaled.append(pivot * inverse)
        head = head - factor * pivot
        value = head if own == 0 else jnp.concatenate([value[: SUB * own], head], axis=0)
    parts = [None] * count
    for a in range(width - 1, -1, -1):
        own, place = a // SUB, a % SUB
        rows = index[:SUB]
        if parts[own] is None:
            parts[own] = jnp.zeros((SUB, right.shape[1]), F32)
        known = jnp.concatenate(parts[own:], axis=0)
        found = scaled[a] - jnp.sum(lower[a] * known, axis=0, keepdims=True)
        parts[own] = jnp.where(rows == place, found, parts[own])
    return jnp.concatenate(parts, axis=0)


def solve_kernel(width, curvature_ref, gradient_ref, out_ref):
    out_ref[...] = solve_packed(
        lambda start, rows: curvature_ref[start : start + rows], gradient_ref[...], width
    )


def newton_solve(curvature, gradient):
    count, width = gradient.shape
    matrix = jnp.transpose(curvature).reshape(width, width, count)
    packed = jnp.concatenate([matrix[a, SUB * (a // SUB) :] for a in range(width)], axis=0)
    fill = -count % LANES
    packed = jnp.pad(packed, ((0, 0), (0, fill)))
    right = jnp.pad(jnp.transpose(gradient), ((0, 0), (0, fill)))
    rows = packed.shape[0]
    result = pl.pallas_call(
        functools.partial(solve_kernel, width),
        grid=((count + fill) // LANES,),
        in_specs=[
            pl.BlockSpec((rows, LANES), lambda i: (0, i)),
            pl.BlockSpec((width, LANES), lambda i: (0, i)),
        ],
        out_specs=pl.BlockSpec((width, LANES), lambda i: (0, i)),
        out_shape=jax.ShapeDtypeStruct(right.shape, F32),
    )(packed, right)
    return jnp.transpose(result[:, :count])


def outer_table(factors):
    width = factors.shape[1]
    product = factors[:, :, None] * factors[:, None, :]
    return product.reshape(factors.shape[0], width * width).astype(BF16)


def predict(offset, factors, loadings):
    linear = offset[:, None] + jnp.dot(factors, loadings.T, precision=HIGH)
    return (linear, jnp.exp(linear))


def gene_contract(counts, expected, loadings):
    weights = expected.astype(BF16)
    residual = (counts.astype(F32) - expected).astype(BF16)
    gradient = jnp.dot(residual, loadings.astype(BF16), preferred_element_type=F32)
    curvature = jnp.dot(weights, outer_table(loadings), preferred_element_type=F32)
    return (gradient, curvature)


def cell_contract(counts, linear, expected, factors):
    counts_real = counts.astype(F32)
    weights = expected.astype(BF16)
    residual = (counts_real - expected).astype(BF16)
    dims = (((0,), (0,)), ((), ()))
    gradient = lax.dot_general(residual, factors.astype(BF16), dims, preferred_element_type=F32)
    curvature = lax.dot_general(weights, outer_table(factors), dims, preferred_element_type=F32)
    terms = 2.0 * (
        counts_real * (jnp.log(jnp.maximum(counts_real, 1.0)) - linear) - counts_real + expected
    )
    return (gradient, curvature, jnp.sum(terms, axis=0))


def by_collectives(counts, totals, cell_factors, gene_loadings):
    offset = jnp.log(totals.astype(F32)) - math.log(SCALE_TOTAL)
    linear, expected = predict(offset, cell_factors, gene_loadings)
    gradient_part, curvature_part = gene_contract(counts, expected, gene_loadings)
    gradient_sum, curvature_sum = lax.psum((gradient_part, curvature_part), "gene")
    new_factors = cell_factors + newton_solve(curvature_sum, gradient_sum - RIDGE * cell_factors)
    cell_total = counts.shape[0] * lax.axis_size("cell")
    linear_next, expected_next = predict(offset, new_factors, gene_loadings)
    gradient_part, curvature_part, deviance_part = cell_contract(
        counts, linear_next, expected_next, new_factors
    )
    gradient_share, curvature_share, deviance_share = (
        lax.psum_scatter(gradient_part, "cell", scatter_dimension=0, tiled=True),
        lax.psum_scatter(curvature_part, "cell", scatter_dimension=0, tiled=True),
        lax.psum_scatter(deviance_part, "cell", scatter_dimension=0, tiled=True),
    )
    portion = gradient_share.shape[0]
    start_row = lax.axis_index("cell") * portion
    own_rows = lax.dynamic_slice_in_dim(gene_loadings, start_row, portion, 0)
    own_new = own_rows + newton_solve(curvature_share, gradient_share - RIDGE * own_rows)
    new_loadings, deviance = (
        lax.all_gather(own_new, "cell", axis=0, tiled=True),
        lax.all_gather(deviance_share / cell_total, "cell", axis=0, tiled=True),
    )
    return (new_factors, new_loadings, deviance)


def send(source, target, send_sem, recv_sem, device):
    return pltpu.make_async_remote_copy(
        src_ref=source,
        dst_ref=target,
        send_sem=send_sem,
        recv_sem=recv_sem,
        device_id=device,
        device_id_type=pl.DeviceIdType.MESH,
    )


def sweep_kernel(
    n_cell,
    n_gene,
    counts_hbm,
    totals_hbm,
    factors_hbm,
    loadings_hbm,
    new_factors_ref,
    new_loadings_ref,
    deviance_ref,
    counts_ref,
    counts_low,
    all_totals,
    factors_ref,
    loads,
    first_own,
    first_in,
    pair_own,
    pair_in,
    total,
    all_factors,
    constant_part,
    second_own,
    second_in,
    deviance_own,
    deviance_in,
    sums,
    local_sem,
    totals_out,
    totals_in,
    loads_out,
    loads_in,
    first_out_sem,
    first_in_sem,
    factors_out,
    factors_in,
    passed_out,
    passed_in,
    second_out_sem,
    second_in_sem,
    deviance_out_sem,
    deviance_in_sem,
    last_out,
    last_in,
):
    cell, gene = lax.axis_index("cell"), lax.axis_index("gene")
    width, cells = factors_ref.shape
    genes = loads.shape[2]
    half = cells // 2
    chunks = genes // BLOCK
    packed = packed_rows(width)

    def flip(index, bits, limit):
        result, bit = 0, 1
        while bit < limit:
            result = result + bit * lax.rem(lax.rem(index // bit, 2) + bits // bit % 2, 2)
            bit *= 2
        return result

    def peer(step):
        return {"cell": flip(cell, step, n_cell), "gene": gene}

    partner = {"cell": cell, "gene": flip(gene, 1, n_gene)}
    across = {"cell": cell, "gene": flip(gene, 2, n_gene)}

    barrier = pltpu.get_barrier_semaphore()
    others = [partner, across] + [peer(step) for step in range(1, n_cell)]
    for other in others:
        pl.semaphore_signal(barrier, inc=1, device_id=other, device_id_type=pl.DeviceIdType.MESH)

    local = [
        pltpu.make_async_copy(loadings_hbm, loads.at[0], local_sem.at[0]),
        pltpu.make_async_copy(totals_hbm, all_totals.at[cell], local_sem.at[1]),
        pltpu.make_async_copy(factors_hbm, factors_ref, local_sem.at[2]),
        pltpu.make_async_copy(counts_hbm, counts_ref, local_sem.at[3]),
    ]
    for copy in local:
        copy.start()

    def chunk(q):
        return pl.ds(pl.multiple_of(q * BLOCK, BLOCK), BLOCK)

    to_partner = send(loads.at[0], loads.at[1], loads_out.at[0], loads_in.at[0], partner)

    def to_across(q):
        return send(
            loads.at[0, :, chunk(q)], loads.at[2, :, chunk(q)], loads_out.at[1 + q], loads_in.at[1 + q], across
        )

    def passed_on(q):
        return send(
            loads.at[2, :, chunk(q)],
            loads.at[3, :, chunk(q)],
            loads_out.at[1 + chunks + q],
            loads_in.at[1 + chunks + q],
            partner,
        )

    def totals_copy(step):
        return send(
            all_totals.at[cell], all_totals.at[cell], totals_out.at[step], totals_in.at[step], peer(step)
        )

    first_copy = send(first_own, first_in, first_out_sem.at[0], first_in_sem.at[0], partner)
    pair_copy = send(pair_own, pair_in, first_out_sem.at[1], first_in_sem.at[1], across)

    local[0].wait()
    local[1].wait()
    with jax.named_scope("z_barrier"):
        pl.semaphore_wait(barrier, len(others))
    for q in range(chunks):
        to_across(q).start()
    to_partner.start()
    for step in range(n_cell - 1, 0, -1):
        totals_copy(step).start()

    local[2].wait()
    offset = jnp.log(all_totals[cell].astype(F32)) - math.log(SCALE_TOTAL)
    with jax.named_scope("a_left"):
        left = fixed_side(factors_ref[...] * LOG2E, rows_of(split3(offset * LOG2E), cells))
    total[...] = jnp.zeros_like(total)
    first_own[...] = jnp.zeros_like(first_own)
    ones = rows_of(1.0, BLOCK)

    def add_genes(slot, q):
        part, extra = accumulate(left, loads[slot, :, chunk(q)], ones)
        total[...] += part
        total[packed:] += extra

    with jax.named_scope("b_countswait"):
        local[3].wait()

    with jax.named_scope("c_counts"):

        @pl.loop(0, chunks)
        def _(q):
            where = chunk(q)
            real = counts_ref[:, where].astype(F32)
            low = real.astype(BF16)
            counts_low[:, where] = low
            constant_part[:, where] = jnp.sum(
                real * jnp.log(jnp.maximum(real, 1.0)) - real, axis=0, keepdims=True
            )
            first_own[...] += lax.dot_general(
                loads[0, :, where].astype(BF16), low, NT, preferred_element_type=F32
            )

    first_copy.start()

    with jax.named_scope("d_own"):

        @pl.loop(0, chunks)
        def _(q):
            add_genes(0, q)

    with jax.named_scope("e_first"):
        first_copy.wait_recv()
        pair_own[...] = first_own[...] + first_in[...]
        pair_copy.start()
        to_partner.wait_recv()

    with jax.named_scope("f_partner"):

        @pl.loop(0, chunks)
        def _(q):
            add_genes(1, q)

    with jax.named_scope("g_wait0"):
        to_across(0).wait_recv()
        passed_on(0).start()
    add_genes(2, 0)

    @pl.loop(1, chunks)
    def _(q):
        with jax.named_scope("g_wait1"):
            to_across(q).wait_recv()
            passed_on(q).start()
        with jax.named_scope("g_add1"):
            add_genes(2, q)
        with jax.named_scope("g_wait2"):
            passed_on(q - 1).wait_recv()
        with jax.named_scope("g_add2"):
            add_genes(3, q - 1)

    with jax.named_scope("g_wait3"):
        passed_on(chunks - 1).wait_recv()
    add_genes(3, chunks - 1)
    with jax.named_scope("g_wait4"):
        pair_copy.wait_recv()

    with jax.named_scope("h_solve1"):
        old = factors_ref[...]
        counted = pair_own[...] + pair_in[...]
        gradient = counted - total[packed : packed + width] - RIDGE * old
        found = old + solve_packed(lambda start, rows: total[start : start + rows], gradient, width)
        new_factors_ref[...] = found
        all_factors[cell] = found

    mine = pl.ds(pl.multiple_of(lax.rem(gene, 2) * half, half), half)
    theirs = pl.ds(pl.multiple_of(half - lax.rem(gene, 2) * half, half), half)

    def factors_copy(step):
        return send(
            new_factors_ref.at[:, mine],
            all_factors.at[cell, :, mine],
            factors_out.at[step],
            factors_in.at[step],
            peer(step),
        )

    def factors_pass(step):
        place = all_factors.at[flip(cell, step, n_cell), :, mine]
        return send(place, place, passed_out.at[step], passed_in.at[step], partner)

    for step in range(n_cell - 1, 0, -1):
        factors_copy(step).start()

    with jax.named_scope("i_second"):
        first, second, _ = split3(new_factors_ref[...])
        stack = jnp.concatenate([first, second, rows_of(split3(offset), cells)], axis=0)

        @pl.loop(0, chunks)
        def _(q):
            where = chunk(q)
            part = jnp.dot(stack, counts_low[:, where], preferred_element_type=F32)
            second_own[:, where] = part[:width]
            whole = loads[0, :, where] * (part[:width] + part[width : 2 * width])
            known = jnp.sum(whole, axis=0, keepdims=True)
            for row in range(3):
                known = known + part[2 * width + row : 2 * width + row + 1]
            deviance_own[:, where] = 2.0 * (constant_part[:, where] - known)

    def lanes(index):
        return pl.ds(pl.multiple_of(index * LANES, LANES), LANES)

    def second_copy(step):
        return send(
            second_own.at[:, lanes(flip(cell, step, n_cell))],
            second_in.at[cell],
            second_out_sem.at[step],
            second_in_sem.at[step],
            peer(step),
        )

    def deviance_copy(step):
        return send(
            deviance_own.at[:, lanes(flip(cell, step, n_cell))],
            deviance_in.at[cell],
            deviance_out_sem.at[step],
            deviance_in_sem.at[step],
            peer(step),
        )

    for step in range(n_cell - 1, 0, -1):
        second_copy(step).start()
        deviance_copy(step).start()

    with jax.named_scope("j_left"):
        own_rows = loads[0, :, lanes(cell)]
        left = fixed_side(own_rows * LOG2E, rows_of(1.0, LANES))
    sums[...] = jnp.zeros_like(sums)

    def add_cells(index):
        offsets = jnp.log(all_totals[index].astype(F32)) - math.log(SCALE_TOTAL)
        part, extra = accumulate(left, all_factors[index], rows_of(split3(offsets * LOG2E), cells))
        sums[...] += part
        sums[packed:] += extra

    with jax.named_scope("k_own"):
        add_cells(cell)

    def take(step):
        totals_copy(step).wait_recv()
        factors_copy(step).wait_recv()
        factors_pass(step).start()

    def passed_to(step):
        place = all_factors.at[flip(cell, step, n_cell), :, theirs]
        return send(place, place, passed_out.at[step], passed_in.at[step], partner)

    with jax.named_scope("l_wait0"):
        take(1)

    for step in range(2, n_cell):
        with jax.named_scope("l_wait1"):
            take(step)
        with jax.named_scope("l_wait2"):
            passed_to(step - 1).wait_recv()
        with jax.named_scope("l_add"):
            add_cells(flip(cell, step - 1, n_cell))
    with jax.named_scope("l_wait3"):
        passed_to(n_cell - 1).wait_recv()
    with jax.named_scope("l_add"):
        add_cells(flip(cell, n_cell - 1, n_cell))

    with jax.named_scope("m_wait"):
        for step in range(1, n_cell):
            second_copy(step).wait_recv()
            deviance_copy(step).wait_recv()

    with jax.named_scope("n_solve2"):
        counted = second_own[:, lanes(cell)]
        deviance = deviance_own[:, lanes(cell)]
        for step in range(1, n_cell):
            counted = counted + second_in[flip(cell, step, n_cell)]
            deviance = deviance + deviance_in[flip(cell, step, n_cell)]
        gradient = counted - sums[packed : packed + width] - RIDGE * own_rows
        new_rows = own_rows + solve_packed(lambda start, rows: sums[start : start + rows], gradient, width)
        plain = sums[packed + width : packed + width + 1]
        new_loadings_ref[:, lanes(cell)] = new_rows
        deviance_ref[:, lanes(cell)] = (deviance + 2.0 * plain) / (cells * n_cell)

    def last_copy(step, which):
        ref = (new_loadings_ref, deviance_ref)[which]
        place = ref.at[:, lanes(cell)]
        return send(place, place, last_out.at[which, step], last_in.at[which, step], peer(step))

    for step in range(n_cell - 1, 0, -1):
        last_copy(step, 0).start()
        last_copy(step, 1).start()
    with jax.named_scope("o_sends"):
        to_partner.wait_send()
        first_copy.wait_send()
        pair_copy.wait_send()
        for q in range(chunks):
            to_across(q).wait_send()
            passed_on(q).wait_send()
        for step in range(1, n_cell):
            totals_copy(step).wait_send()
            factors_copy(step).wait_send()
            factors_pass(step).wait_send()
            second_copy(step).wait_send()
            deviance_copy(step).wait_send()
    with jax.named_scope("p_last"):
        for step in range(1, n_cell):
            last_copy(step, 0).wait_send()
            last_copy(step, 1).wait_send()
        for step in range(1, n_cell):
            last_copy(step, 0).wait_recv()
            last_copy(step, 1).wait_recv()


def finish_kernel(*refs):
    count = len(refs) // 2
    sem = refs[-1]
    copies = [pltpu.make_async_copy(refs[i], refs[count + i], sem.at[i]) for i in range(count)]
    for copy in copies:
        copy.start()
    for copy in copies:
        copy.wait()


def by_kernel(n_cell, n_gene, counts, totals, cell_factors, gene_loadings):
    cells, genes = counts.shape
    width = cell_factors.shape[1]
    rows = packed_rows(width) + width + 2 * SUB
    chunks = genes // BLOCK
    vmem = pl.BlockSpec(memory_space=pltpu.VMEM)
    hbm = pl.BlockSpec(memory_space=pltpu.HBM)
    dma = lambda *n: pltpu.SemaphoreType.DMA(n)
    shapes = (
        jax.ShapeDtypeStruct((width, cells), F32),
        jax.ShapeDtypeStruct((width, genes), F32),
        jax.ShapeDtypeStruct((1, genes), F32),
    )
    results = pl.pallas_call(
        functools.partial(sweep_kernel, n_cell, n_gene),
        out_shape=shapes,
        in_specs=[hbm] * 4,
        out_specs=(vmem,) * 3,
        scratch_shapes=[
            pltpu.VMEM((cells, genes), jnp.int32),
            pltpu.VMEM((cells, genes), BF16),
            pltpu.VMEM((n_cell, 1, cells), jnp.int32),
            pltpu.VMEM((width, cells), F32),
            pltpu.VMEM((n_gene, width, genes), F32),
            pltpu.VMEM((width, cells), F32),
            pltpu.VMEM((width, cells), F32),
            pltpu.VMEM((width, cells), F32),
            pltpu.VMEM((width, cells), F32),
            pltpu.VMEM((rows, cells), F32),
            pltpu.VMEM((n_cell, width, cells), F32),
            pltpu.VMEM((1, genes), F32),
            pltpu.VMEM((width, genes), F32),
            pltpu.VMEM((n_cell, width, LANES), F32),
            pltpu.VMEM((1, genes), F32),
            pltpu.VMEM((n_cell, 1, LANES), F32),
            pltpu.VMEM((rows, LANES), F32),
            dma(4),
            dma(n_cell),
            dma(n_cell),
            dma(1 + 2 * chunks),
            dma(1 + 2 * chunks),
            dma(2),
            dma(2),
            dma(n_cell),
            dma(n_cell),
            dma(n_cell),
            dma(n_cell),
            dma(n_cell),
            dma(n_cell),
            dma(n_cell),
            dma(n_cell),
            dma(2, n_cell),
            dma(2, n_cell),
        ],
        compiler_params=pltpu.CompilerParams(
            collective_id=0, has_side_effects=True, vmem_limit_bytes=24000 * 1024
        ),
    )(counts, totals.reshape(1, cells), cell_factors.T, gene_loadings.T)
    new_factors, new_loadings, deviance = pl.pallas_call(
        finish_kernel,
        out_shape=shapes,
        in_specs=[vmem] * 3,
        out_specs=(hbm,) * 3,
        scratch_shapes=[dma(3)],
        compiler_params=pltpu.CompilerParams(vmem_limit_bytes=8000 * 1024),
    )(*results)
    return (new_factors.T, new_loadings.T, deviance.reshape(genes))


def solution(mesh):
    n_cell, n_gene = mesh.shape["cell"], mesh.shape["gene"]

    def on_device(counts, totals, cell_factors, gene_loadings):
        cells, genes = counts.shape
        whole_lanes = genes == n_cell * LANES and cells == 2 * LANES and genes % BLOCK == 0
        if whole_lanes and n_gene == 4 and n_cell & (n_cell - 1) == 0:
            return by_kernel(n_cell, n_gene, counts, totals, cell_factors, gene_loadings)
        return by_collectives(counts, totals, cell_factors, gene_loadings)

    return jax.shard_map(
        on_device,
        mesh=mesh,
        in_specs=(P("cell", "gene"), P("cell"), P("cell", None), P("gene", None)),
        out_specs=(P("cell", None), P("gene", None), P("gene")),
        check_vma=False,
    )
```

```python
import functools
import math

import jax
import jax.numpy as jnp
from jax import lax
from jax.experimental import pallas as pl
from jax.experimental.pallas import tpu as pltpu
from jax.sharding import PartitionSpec as P

RIDGE = 1.0
DAMPING = 0.1
SCALE_TOTAL = 5000.0
LANES = 128
SUB = 8
BLOCK = 256
HIGH = lax.Precision.HIGHEST
NT = (((1,), (1,)), ((), ()))
LOG2E = 1.0 / math.log(2.0)
F32 = jnp.float32
BF16 = jnp.bfloat16


def packed_rows(width):
    return sum(width - SUB * (a // SUB) for a in range(width))


def lower_table(factors):
    width = factors.shape[0]
    pieces = [factors[a : a + 1] * factors[SUB * (a // SUB) :] for a in range(width)]
    return jnp.concatenate(pieces, axis=0).astype(BF16)


def split3(x):
    first = x.astype(BF16)
    rest = x - first.astype(F32)
    second = rest.astype(BF16)
    third = (rest - second.astype(F32)).astype(BF16)
    return first, second, third


def rows_of(value, count):
    index = lax.broadcasted_iota(jnp.int32, (2 * SUB, count), 0)
    parts = [x.astype(F32) for x in value] if isinstance(value, tuple) else [value] * 3
    result = jnp.zeros((2 * SUB, count), F32)
    for place, part in enumerate(parts):
        result = jnp.where(index == place, part, result)
    return result.astype(BF16)


def fixed_side(rows, tail):
    first, second, third = (x.astype(F32) for x in split3(rows))
    stack = jnp.concatenate([first, first, second, first, third, second, tail.astype(F32)], axis=0)
    return jnp.transpose(stack).astype(BF16)


def stream_side(rows, tail):
    first, second, third = split3(rows)
    return jnp.concatenate([first, second, first, third, first, second, tail], axis=0), first


def table_of(rows, first):
    width, count = rows.shape
    ones = jnp.where(lax.broadcasted_iota(jnp.int32, (2 * SUB, count), 0) == 0, 1.0, 0.0).astype(BF16)
    return jnp.concatenate([lower_table(rows), first, ones], axis=0)


def accumulate(left, rows, tail):
    width = rows.shape[0]
    right, first = stream_side(rows, tail)
    expected = jnp.exp2(jnp.dot(left, right, preferred_element_type=F32))
    high = expected.astype(BF16)
    low = (expected - high.astype(F32)).astype(BF16)
    table = table_of(rows, first)
    sums = lax.dot_general(table, high, NT, preferred_element_type=F32)
    extra = lax.dot_general(table[packed_rows(width) :], low, NT, preferred_element_type=F32)
    return sums, extra


def solve_packed(get, right, width, lower_ref):
    columns, start = [], 0
    groups = right.shape[1] // LANES
    for a in range(width):
        rows = width - SUB * (a // SUB)
        columns.append(get(start, rows))
        start += rows
    diagonal = sum(columns[a][a % SUB : a % SUB + 1] for a in range(width)) / width
    shift = RIDGE + DAMPING * diagonal
    count = width // SUB
    index = lax.broadcasted_iota(jnp.int32, (width, right.shape[1]), 0)
    scaled = []
    value = right
    for a in range(width):
        own, place = a // SUB, a % SUB
        column = columns[a]
        rows = index[: width - SUB * own]
        inverse = 1.0 / (column[place : place + 1] + shift)
        factor = jnp.where(rows > place, column * inverse, 0.0)
        for b in range(a + 1, width):
            offset = SUB * (b // SUB - own)
            coefficient = column[b - SUB * own : b - SUB * own + 1]
            columns[b] = columns[b] - factor[offset:] * coefficient
        for group in range(groups):
            lower_ref[group, width * a + SUB * own : width * (a + 1)] = factor[
                :, group * LANES : (group + 1) * LANES
            ]
        head = value[SUB * own :]
        pivot = head[place : place + 1]
        scaled.append(pivot * inverse)
        head = head - factor * pivot
        value = head if own == 0 else jnp.concatenate([value[: SUB * own], head], axis=0)
    stripe = index[:SUB]
    parts = []
    for block in range(count):
        part = jnp.zeros((SUB, right.shape[1]), F32)
        for place in range(SUB):
            part = jnp.where(stripe == place, scaled[SUB * block + place], part)
        parts.append(part)
    for a in range(width - 1, 0, -1):
        own, place = a // SUB, a % SUB
        found = parts[own][place : place + 1]
        for block in range(own + (place > 0)):
            rows = pl.ds(SUB * block * width + a, SUB, stride=width)
            row = jnp.concatenate([lower_ref[group, rows, :] for group in range(groups)], axis=1)
            parts[block] = parts[block] - row * found
    return jnp.concatenate(parts, axis=0)


def solve_kernel(width, curvature_ref, gradient_ref, out_ref, lower_ref):
    out_ref[...] = solve_packed(
        lambda start, rows: curvature_ref[start : start + rows], gradient_ref[...], width, lower_ref
    )


def newton_solve(curvature, gradient):
    count, width = gradient.shape
    matrix = jnp.transpose(curvature).reshape(width, width, count)
    packed = jnp.concatenate([matrix[a, SUB * (a // SUB) :] for a in range(width)], axis=0)
    fill = -count % LANES
    packed = jnp.pad(packed, ((0, 0), (0, fill)))
    right = jnp.pad(jnp.transpose(gradient), ((0, 0), (0, fill)))
    rows = packed.shape[0]
    result = pl.pallas_call(
        functools.partial(solve_kernel, width),
        grid=((count + fill) // LANES,),
        in_specs=[
            pl.BlockSpec((rows, LANES), lambda i: (0, i)),
            pl.BlockSpec((width, LANES), lambda i: (0, i)),
        ],
        out_specs=pl.BlockSpec((width, LANES), lambda i: (0, i)),
        out_shape=jax.ShapeDtypeStruct(right.shape, F32),
        scratch_shapes=[pltpu.VMEM((1, width * width, LANES), F32)],
    )(packed, right)
    return jnp.transpose(result[:, :count])


def outer_table(factors):
    width = factors.shape[1]
    product = factors[:, :, None] * factors[:, None, :]
    return product.reshape(factors.shape[0], width * width).astype(BF16)


def predict(offset, factors, loadings):
    linear = offset[:, None] + jnp.dot(factors, loadings.T, precision=HIGH)
    return (linear, jnp.exp(linear))


def gene_contract(counts, expected, loadings):
    weights = expected.astype(BF16)
    residual = (counts.astype(F32) - expected).astype(BF16)
    gradient = jnp.dot(residual, loadings.astype(BF16), preferred_element_type=F32)
    curvature = jnp.dot(weights, outer_table(loadings), preferred_element_type=F32)
    return (gradient, curvature)


def cell_contract(counts, linear, expected, factors):
    counts_real = counts.astype(F32)
    weights = expected.astype(BF16)
    residual = (counts_real - expected).astype(BF16)
    dims = (((0,), (0,)), ((), ()))
    gradient = lax.dot_general(residual, factors.astype(BF16), dims, preferred_element_type=F32)
    curvature = lax.dot_general(weights, outer_table(factors), dims, preferred_element_type=F32)
    terms = 2.0 * (
        counts_real * (jnp.log(jnp.maximum(counts_real, 1.0)) - linear) - counts_real + expected
    )
    return (gradient, curvature, jnp.sum(terms, axis=0))


def by_collectives(counts, totals, cell_factors, gene_loadings):
    offset = jnp.log(totals.astype(F32)) - math.log(SCALE_TOTAL)
    linear, expected = predict(offset, cell_factors, gene_loadings)
    gradient_part, curvature_part = gene_contract(counts, expected, gene_loadings)
    gradient_sum, curvature_sum = lax.psum((gradient_part, curvature_part), "gene")
    new_factors = cell_factors + newton_solve(curvature_sum, gradient_sum - RIDGE * cell_factors)
    cell_total = counts.shape[0] * lax.axis_size("cell")
    linear_next, expected_next = predict(offset, new_factors, gene_loadings)
    gradient_part, curvature_part, deviance_part = cell_contract(
        counts, linear_next, expected_next, new_factors
    )
    gradient_share, curvature_share, deviance_share = (
        lax.psum_scatter(gradient_part, "cell", scatter_dimension=0, tiled=True),
        lax.psum_scatter(curvature_part, "cell", scatter_dimension=0, tiled=True),
        lax.psum_scatter(deviance_part, "cell", scatter_dimension=0, tiled=True),
    )
    portion = gradient_share.shape[0]
    start_row = lax.axis_index("cell") * portion
    own_rows = lax.dynamic_slice_in_dim(gene_loadings, start_row, portion, 0)
    own_new = own_rows + newton_solve(curvature_share, gradient_share - RIDGE * own_rows)
    new_loadings, deviance = (
        lax.all_gather(own_new, "cell", axis=0, tiled=True),
        lax.all_gather(deviance_share / cell_total, "cell", axis=0, tiled=True),
    )
    return (new_factors, new_loadings, deviance)


def send(source, target, send_sem, recv_sem, device):
    return pltpu.make_async_remote_copy(
        src_ref=source,
        dst_ref=target,
        send_sem=send_sem,
        recv_sem=recv_sem,
        device_id=device,
        device_id_type=pl.DeviceIdType.MESH,
    )


def sweep_kernel(
    n_cell,
    n_gene,
    counts_hbm,
    totals_hbm,
    factors_hbm,
    loadings_hbm,
    new_factors_ref,
    new_loadings_ref,
    deviance_ref,
    counts_ref,
    counts_low,
    all_totals,
    factors_ref,
    loads,
    first_own,
    first_in,
    pair_own,
    pair_in,
    total,
    all_factors,
    constant_part,
    second_own,
    second_in,
    deviance_own,
    deviance_in,
    sums,
    lower_ref,
    local_sem,
    send_sem,
    once_in,
    loads_in,
    factors_in,
    relay_in,
    passed_in,
):
    cell, gene = lax.axis_index("cell"), lax.axis_index("gene")
    width, cells = factors_ref.shape
    genes = loads.shape[2]
    half = cells // 2
    chunks = genes // BLOCK
    packed = packed_rows(width)

    def flip(index, bits, limit):
        result, bit = 0, 1
        while bit < limit:
            result = result + bit * lax.rem(lax.rem(index // bit, 2) + bits // bit % 2, 2)
            bit *= 2
        return result

    def near(step):
        return flip(cell, step, n_cell)

    def peer(step):
        return {"cell": near(step), "gene": gene}

    def lanes(index):
        return pl.ds(pl.multiple_of(index * LANES, LANES), LANES)

    def chunk(q):
        return slice(q * BLOCK, (q + 1) * BLOCK)

    def take_all(view, sem):
        pltpu.make_async_copy(view, view, sem).wait()

    partner = {"cell": cell, "gene": flip(gene, 1, n_gene)}
    across = {"cell": cell, "gene": flip(gene, 2, n_gene)}
    core = lax.rem(gene, 2)
    mine, theirs = lanes(core), lanes(1 - core)
    out_totals, out_across, out_partner, out_passed, out_first, out_pair = (send_sem.at[k] for k in range(6))
    out_own, out_factors, out_relay, out_turn, out_second, out_deviance = (send_sem.at[k] for k in range(6, 12))
    out_last, out_tail = (send_sem.at[k] for k in range(12, 14))
    in_totals, in_first, in_pair, in_own = (once_in.at[k] for k in range(4))
    in_second, in_deviance, in_last, in_tail = (once_in.at[k] for k in range(4, 8))
    steps = list(range(n_cell - 1, 0, -1))
    far = [step for step in steps if step % 2 == 0]

    barrier = pltpu.get_barrier_semaphore()
    others = [partner, across] + [peer(step) for step in steps]
    for other in others:
        pl.semaphore_signal(barrier, inc=1, device_id=other, device_id_type=pl.DeviceIdType.MESH)

    local = [
        pltpu.make_async_copy(loadings_hbm, loads.at[0], local_sem.at[0]),
        pltpu.make_async_copy(totals_hbm, all_totals.at[cell], local_sem.at[1]),
        pltpu.make_async_copy(factors_hbm, factors_ref, local_sem.at[2]),
        pltpu.make_async_copy(counts_hbm, counts_ref, local_sem.at[3]),
    ]
    for copy in local:
        copy.start()

    to_partner = send(loads.at[0], loads.at[1], out_partner, loads_in.at[0], partner)

    def to_across(q):
        return send(loads.at[0, :, chunk(q)], loads.at[2, :, chunk(q)], out_across, loads_in.at[1 + q], across)

    def passed_on(q):
        where = chunk(q)
        return send(loads.at[2, :, where], loads.at[3, :, where], out_passed, loads_in.at[1 + chunks + q], partner)

    local[0].wait()
    local[1].wait()
    with jax.named_scope("z_barrier"):
        pl.semaphore_wait(barrier, len(others))
    for q in range(chunks):
        to_across(q).start()
    to_partner.start()
    for step in steps:
        send(all_totals.at[cell], all_totals.at[cell], out_totals, in_totals, peer(step)).start()

    local[2].wait()
    offset = jnp.log(all_totals[cell].astype(F32)) - math.log(SCALE_TOTAL)
    own_offset = jnp.log(all_totals[cell, :, mine].astype(F32)) - math.log(SCALE_TOTAL)
    old = factors_ref[:, mine]
    with jax.named_scope("a_left"):
        left = fixed_side(old * LOG2E, rows_of(split3(own_offset * LOG2E), LANES))

    def add_genes(slot, begin, count):
        part, extra = accumulate(left, loads[slot, :, begin : begin + count], rows_of(1.0, count))
        total[...] += part
        total[packed:] += extra

    with jax.named_scope("b_own"):
        part, extra = accumulate(left, loads[0], rows_of(1.0, genes))
        total[...] = part
        total[packed:] += extra

    with jax.named_scope("c_counts"):
        local[3].wait()
        real = counts_ref[...].astype(F32)
        low = real.astype(BF16)
        counts_low[...] = low
        constant_part[...] = jnp.sum(real * jnp.log(jnp.maximum(real, 1.0)) - real, axis=0, keepdims=True)
        first_own[...] = lax.dot_general(loads[0].astype(BF16), low, NT, preferred_element_type=F32)
    first_copy = send(first_own.at[:, theirs], first_in, out_first, in_first, partner)
    first_copy.start()
    own_rows = loads[0, :, lanes(cell)]
    second_left = fixed_side(own_rows * LOG2E, rows_of(1.0, LANES))

    with jax.named_scope("e_first"):
        to_partner.wait_recv()
    with jax.named_scope("f_partner"):
        add_genes(1, 0, genes)
        first_copy.wait_recv()
        pair_own[...] = first_own[:, mine] + first_in[...]
        pair_copy = send(pair_own, pair_in, out_pair, in_pair, across)
        pair_copy.start()

    def arrive(q):
        with jax.named_scope("g_wait_y"):
            to_across(q).wait_recv()
            passed_on(q).start()

    def arrive_passed(q):
        with jax.named_scope("g_wait_p"):
            passed_on(q).wait_recv()

    arrive(0)
    arrive(1)
    with jax.named_scope("g_add"):
        add_genes(2, 0, 2 * BLOCK)
    arrive(2)
    arrive_passed(0)
    arrive_passed(1)
    with jax.named_scope("g_add"):
        add_genes(3, 0, 2 * BLOCK)
    arrive(3)
    with jax.named_scope("g_add"):
        add_genes(2, 2 * BLOCK, 2 * BLOCK)
    arrive_passed(2)
    with jax.named_scope("g_add"):
        add_genes(3, 2 * BLOCK, BLOCK)
    arrive_passed(3)
    with jax.named_scope("g_add"):
        add_genes(3, 3 * BLOCK, BLOCK)
    with jax.named_scope("g_wait_pair"):
        pair_copy.wait_recv()

    with jax.named_scope("h_solve1"):
        counted = pair_own[...] + pair_in[...]
        gradient = counted - total[packed : packed + width] - RIDGE * old
        found = old + solve_packed(
            lambda start, rows: total[start : start + rows], gradient, width, lower_ref
        )
        all_factors[cell, :, mine] = found

    def factors_copy(step):
        place = all_factors.at[cell, :, mine]
        return send(place, place, out_factors, factors_in.at[step // 2], peer(step))

    def factors_relay(step):
        place = all_factors.at[near(step), :, mine]
        return send(place, place, out_relay, relay_in.at[step // 2 - 1], peer(1))

    def factors_relayed(step):
        place = all_factors.at[near(step + 1), :, mine]
        return send(place, place, out_relay, relay_in.at[step // 2 - 1], peer(1))

    def factors_pass(step, place):
        place = all_factors.at[near(step), :, place]
        return send(place, place, out_turn, passed_in.at[step - 1], partner)

    place = all_factors.at[cell, :, mine]
    own_pass = send(place, place, out_own, in_own, partner)
    for step in far + [1]:
        factors_copy(step).start()
    own_pass.start()

    def sum_cells(index, where=slice(None)):
        offsets = jnp.log(all_totals[index, :, where].astype(F32)) - math.log(SCALE_TOTAL)
        rows = all_factors[index, :, where]
        return accumulate(second_left, rows, rows_of(split3(offsets * LOG2E), rows.shape[1]))

    def add_cells(index, where=slice(None)):
        part, extra = sum_cells(index, where)
        sums[...] += part
        sums[packed:] += extra

    with jax.named_scope("k_own1"):
        part, extra = sum_cells(cell, mine)
        sums[...] = part
        sums[packed:] += extra

    with jax.named_scope("i_wait"):
        own_pass.wait_recv()
    with jax.named_scope("i_second"):
        first, second, _ = split3(all_factors[cell])
        stack = jnp.concatenate([first, second, rows_of(split3(offset), cells)], axis=0)
        part = jnp.dot(stack, counts_low[...], preferred_element_type=F32)
        second_own[...] = part[:width]
        whole = loads[0] * (part[:width] + part[width : 2 * width])
        known = jnp.sum(whole, axis=0, keepdims=True)
        for row in range(3):
            known = known + part[2 * width + row : 2 * width + row + 1]
        deviance_own[...] = 2.0 * (constant_part[...] - known)

    for step in steps:
        where = lanes(near(step))
        send(second_own.at[:, where], second_in.at[step - 1], out_second, in_second, peer(step)).start()
        send(deviance_own.at[:, where], deviance_in.at[step - 1], out_deviance, in_deviance, peer(step)).start()

    with jax.named_scope("k_own2"):
        add_cells(cell, theirs)
        new_factors_ref[...] = all_factors[cell]
        take_all(all_totals.at[pl.ds(0, n_cell - 1)], in_totals)

    def take(step):
        if step == 1 or step % 2 == 0:
            factors_copy(step).wait_recv()
            if step > 1:
                factors_relay(step).start()
        else:
            factors_relayed(step - 1).wait_recv()
        factors_pass(step, mine).start()

    order = [2, 1] + far[::-1][1:] + [step + 1 for step in far[::-1]]
    with jax.named_scope("l_wait0"):
        take(order[0])
    for index, step in enumerate(order):
        if index + 1 < len(order):
            with jax.named_scope("l_wait1"):
                take(order[index + 1])
        with jax.named_scope("l_wait2"):
            factors_pass(step, theirs).wait_recv()
        with jax.named_scope("l_add"):
            add_cells(near(step))

    with jax.named_scope("m_wait"):
        take_all(second_in, in_second)
        take_all(deviance_in, in_deviance)

    with jax.named_scope("n_solve2"):
        counted = second_own[:, lanes(cell)]
        deviance = deviance_own[:, lanes(cell)]
        for step in steps:
            counted = counted + second_in[step - 1]
            deviance = deviance + deviance_in[step - 1]
        gradient = counted - sums[packed : packed + width] - RIDGE * own_rows
        new_rows = own_rows + solve_packed(
            lambda start, rows: sums[start : start + rows], gradient, width, lower_ref
        )
        plain = sums[packed + width : packed + width + 1]
        new_loadings_ref[:, lanes(cell)] = new_rows
        deviance_ref[:, lanes(cell)] = (deviance + 2.0 * plain) / (cells * n_cell)

    for step in steps:
        place = new_loadings_ref.at[:, lanes(cell)]
        send(place, place, out_last, in_last, peer(step)).start()
        place = deviance_ref.at[:, lanes(cell)]
        send(place, place, out_tail, in_tail, peer(step)).start()
    with jax.named_scope("o_sends"):
        to_partner.wait_send()
        first_copy.wait_send()
        pair_copy.wait_send()
        own_pass.wait_send()
        take_all(all_totals.at[pl.ds(0, n_cell - 1)], out_totals)
        take_all(loads.at[0], out_across)
        take_all(loads.at[0], out_passed)
        take_all(second_in.at[pl.ds(0, len(far) + 1)], out_factors)
        take_all(second_in.at[pl.ds(0, len(far))], out_relay)
        take_all(second_in, out_turn)
        take_all(second_in, out_second)
        take_all(deviance_in, out_deviance)
    with jax.named_scope("p_last"):
        take_all(second_in, out_last)
        take_all(deviance_in, out_tail)
        take_all(second_in, in_last)
        take_all(deviance_in, in_tail)


def finish_kernel(*refs):
    count = len(refs) // 2
    sem = refs[-1]
    copies = [pltpu.make_async_copy(refs[i], refs[count + i], sem.at[i]) for i in range(count)]
    for copy in copies:
        copy.start()
    for copy in copies:
        copy.wait()


def by_kernel(n_cell, n_gene, counts, totals, cell_factors, gene_loadings):
    cells, genes = counts.shape
    width = cell_factors.shape[1]
    rows = packed_rows(width) + width + 2 * SUB
    chunks = genes // BLOCK
    vmem = pl.BlockSpec(memory_space=pltpu.VMEM)
    hbm = pl.BlockSpec(memory_space=pltpu.HBM)
    dma = lambda *n: pltpu.SemaphoreType.DMA(n)
    shapes = (
        jax.ShapeDtypeStruct((width, cells), F32),
        jax.ShapeDtypeStruct((width, genes), F32),
        jax.ShapeDtypeStruct((1, genes), F32),
    )
    inputs = (counts, totals.reshape(1, cells), cell_factors.T, gene_loadings.T)
    results = pl.pallas_call(
        functools.partial(sweep_kernel, n_cell, n_gene),
        out_shape=shapes,
        in_specs=[hbm] * 4,
        out_specs=(vmem,) * 3,
        scratch_shapes=[
            pltpu.VMEM((cells, genes), jnp.int32),
            pltpu.VMEM((cells, genes), BF16),
            pltpu.VMEM((n_cell, 1, cells), jnp.int32),
            pltpu.VMEM((width, cells), F32),
            pltpu.VMEM((n_gene, width, genes), F32),
            pltpu.VMEM((width, cells), F32),
            pltpu.VMEM((width, LANES), F32),
            pltpu.VMEM((width, LANES), F32),
            pltpu.VMEM((width, LANES), F32),
            pltpu.VMEM((rows, LANES), F32),
            pltpu.VMEM((n_cell, width, cells), F32),
            pltpu.VMEM((1, genes), F32),
            pltpu.VMEM((width, genes), F32),
            pltpu.VMEM((n_cell - 1, width, LANES), F32),
            pltpu.VMEM((1, genes), F32),
            pltpu.VMEM((n_cell - 1, 1, LANES), F32),
            pltpu.VMEM((rows, LANES), F32),
            pltpu.VMEM((1, width * width, LANES), F32),
            dma(4),
            dma(14),
            dma(8),
            dma(1 + 2 * chunks),
            dma(n_cell // 2),
            dma(n_cell // 2 - 1),
            dma(n_cell - 1),
        ],
        compiler_params=pltpu.CompilerParams(
            collective_id=0, has_side_effects=True, vmem_limit_bytes=24000 * 1024
        ),
    )(*[pltpu.with_memory_space_constraint(x, pltpu.HBM) for x in inputs])
    new_factors, new_loadings, deviance = pl.pallas_call(
        finish_kernel,
        out_shape=shapes,
        in_specs=[vmem] * 3,
        out_specs=(hbm,) * 3,
        scratch_shapes=[dma(3)],
        compiler_params=pltpu.CompilerParams(vmem_limit_bytes=8000 * 1024),
    )(*results)
    return (new_factors.T, new_loadings.T, deviance.reshape(genes))


def solution(mesh):
    n_cell, n_gene = mesh.shape["cell"], mesh.shape["gene"]

    def on_device(counts, totals, cell_factors, gene_loadings):
        cells, genes = counts.shape
        whole_lanes = genes == n_cell * LANES and cells == 2 * LANES and genes % BLOCK == 0
        if whole_lanes and n_gene == 4 and n_cell & (n_cell - 1) == 0:
            return by_kernel(n_cell, n_gene, counts, totals, cell_factors, gene_loadings)
        return by_collectives(counts, totals, cell_factors, gene_loadings)

    return jax.shard_map(
        on_device,
        mesh=mesh,
        in_specs=(P("cell", "gene"), P("cell"), P("cell", None), P("gene", None)),
        out_specs=(P("cell", None), P("gene", None), P("gene")),
        check_vma=False,
    )
```
